32 devices in a mesh: ep: 8 (over y, x, core), tp: 4 (over z).
Axes of the slice: x: 2, y: 2, z: 4, core: 2. Of those that a mesh axis runs over, the one named last changes fastest.
Arguments:
- tokens: bfloat16 [2048, 7168], P('ep', 'tp'), may hold values from -78 to 78
- norm_gain: bfloat16 [7168], P('tp'), may hold values from 0.5 to 1.5
- expert_ids: int32 [2048, 8], P('ep'), may hold values from 0 to 63, all different within a row
- gate_prob: bfloat16 [2048, 8], P('ep'), may hold values from 0.049804688 to 1
- w_gate: bfloat16 [8, 7168, 2048], P('ep', None, 'tp'), may hold values from -0.0625 to 0.0625
- w_up: bfloat16 [8, 7168, 2048], P('ep', None, 'tp'), may hold values from -0.0625 to 0.0625
- w_down: bfloat16 [8, 2048, 7168], P('ep', 'tp'), may hold values from -0.125 to 0.125
Outputs:
- combined: bfloat16 [2048, 7168], P('ep', 'tp')
The draws below stay inside these ranges and needn't reach their ends.
Inputs may be any that keep to these rules, and one draw needn't show every extreme that they name: `expert_ids`: each row names 8 different experts.
All inputs are finite; a program needn't handle non-finite values.
Results may differ from the reference program's by a relative error of at most 0.01.
Values may be sent and summed in bfloat16 or wider, within the bound.
A program may use at most 128 MiB of HBM per device.

```python
import math
import jax
import jax.numpy as jnp
from jax import lax

D = 7168
FF = 2048
TOP = 8
TOK_DEV = 256
EXPERTS = 64
WINDOW = 8
TOKENS = 2048
CAP = 64
N_TP = 4


def draw_tokens(key, part):
    base_key = jax.random.fold_in(key, 11)
    row_key = jax.random.fold_in(key, 12)
    col_key = jax.random.fold_in(key, 13)
    rows_scale = jnp.exp(jax.random.uniform(row_key, (TOKENS, 1), jnp.float32, math.log(0.3), math.log(3.0)))
    rising = 3.0 ** (jnp.arange(D, dtype=jnp.float32) / D - 0.5)
    cols_scale = rising * jnp.exp(jax.random.uniform(col_key, (D,), jnp.float32, math.log(0.4), math.log(2.5)))
    base = jnp.clip(jax.random.normal(base_key, (TOKENS, D), jnp.float32), -6.0, 6.0)
    return (base * rows_scale * cols_scale[None, :]).astype(jnp.bfloat16)


def block_levels(key, shape, pieces, low, largest):
    def one(dim, shards_of):
        heights = jax.random.uniform(jax.random.fold_in(jax.random.fold_in(key, 6), dim), (shards_of,), jnp.float32, low / len(pieces), largest / len(pieces))
        return jnp.repeat(jnp.exp(heights), shape[dim] // shards_of).reshape((-1,) + (1,) * (len(shape) - dim - 1))

    factor_of = one(*pieces[0])
    for cut in pieces[1:]:
        factor_of = factor_of * one(*cut)
    return factor_of


def distinct(own_key, rows, amount, top, lift):
    sequence = jax.random.permutation(jax.random.fold_in(own_key, 1), amount)
    boost = sequence
    for power in range(3):
        boost = boost * boost // amount
    boost = boost * lift // amount
    lots = jax.random.randint(jax.random.fold_in(own_key, 2), (rows, amount), 0, 4096) + boost
    sure = jax.random.permutation(jax.random.fold_in(own_key, 3), rows)[jnp.arange(amount) % rows]
    lots = jnp.where(jnp.arange(rows)[:, None] == sure[None, :], 1 << 14, lots)
    score = lots * amount + jnp.arange(amount)
    return lax.top_k(score.astype(jnp.int32), top)[1].astype(jnp.int32)


def noise(own_key, shape, width, reach, shards=(), kind=jnp.bfloat16):
    array = jax.random.normal(own_key, shape, jnp.float32) * width
    if len(shards) > 0:
        array = block_levels(own_key, shape, shards, -0.22, 0.18) * array
    return jnp.clip(array, min=-reach, max=reach).astype(kind)


def setup_inputs(seed: int = 0) -> dict:
    arg_keys = jax.random.split(jax.random.key(seed), 8)
    tokens = draw_tokens(jax.random.fold_in(arg_keys[7], 71), 0)
    norm_gain = jnp.clip(1.0 + 0.1 * jax.random.normal(arg_keys[1], (D,), jnp.float32), 0.5, 1.5).astype(jnp.bfloat16)
    expert_ids = distinct(arg_keys[2], TOKENS, EXPERTS, TOP, 2048)
    gate_prob = jnp.clip(jnp.exp(math.log(1.0) - 2.9996462 * jax.random.uniform(arg_keys[3], (TOKENS, TOP), jnp.float32) ** block_levels(arg_keys[3], (TOKENS, TOP), ((0, 8),), -0.2, 0.2)), 0.049804688, 1.0).astype(jnp.bfloat16)
    w_gate = noise(arg_keys[4], (WINDOW, D, FF), D ** -0.5, 0.0625, ((0, 8), (2, 4)))
    w_up = noise(arg_keys[5], (WINDOW, D, FF), D ** -0.5, 0.0625, ((0, 8), (2, 4)))
    w_down = noise(arg_keys[6], (WINDOW, FF, D), FF ** -0.5, 0.125, ((0, 8), (1, 4)))
    return dict(tokens=tokens, norm_gain=norm_gain, expert_ids=expert_ids, gate_prob=gate_prob, w_gate=w_gate, w_up=w_up, w_down=w_down)


epsilon = 1e-06

def slots_of(expert_ids):
    is_live = expert_ids < WINDOW
    matches = (expert_ids[:, :, None] == jnp.arange(WINDOW, dtype=jnp.int32)).astype(jnp.int32)
    counts = lax.optimization_barrier(jnp.sum(matches, axis=1))
    blocked = counts.reshape(-1, TOK_DEV, WINDOW)
    before = (jnp.cumsum(blocked, axis=1) - blocked).reshape(-1, WINDOW)
    slot_index = lax.optimization_barrier(jnp.sum(matches * before[:, None, :], axis=2))
    is_kept = is_live & (slot_index < CAP)
    return (slot_index, is_kept)

def reference(tokens, norm_gain, expert_ids, gate_prob, w_gate, w_up, w_down):
    values = tokens.astype(jnp.float32)
    mean_square = lax.optimization_barrier(jnp.mean(values * values, axis=1, keepdims=True))
    normed = (values * lax.rsqrt(mean_square + epsilon) * norm_gain.astype(jnp.float32)).astype(jnp.bfloat16)
    slot_index, is_kept = slots_of(expert_ids)
    block_count = TOKENS // TOK_DEV
    block_index = (jnp.arange(TOKENS, dtype=jnp.int32) // TOK_DEV)[:, None]
    slot_total = WINDOW * block_count * CAP
    flat_index = jnp.where(is_kept, (expert_ids * block_count + block_index) * CAP + slot_index, slot_total).astype(jnp.int32)
    buffer = jnp.zeros((slot_total, D), jnp.bfloat16)
    for column in range(TOP):
        buffer = buffer.at[flat_index[:, column]].set(normed, mode='drop')
    buffer = buffer.reshape(WINDOW, block_count * CAP, D)
    block_width = FF // N_TP

    def one_expert(operands):
        rows_in, gate_matrix, up_matrix, down_matrix = operands
        gate_act = jnp.dot(rows_in, gate_matrix, preferred_element_type=jnp.float32)
        up_act = jnp.dot(rows_in, up_matrix, preferred_element_type=jnp.float32)
        hidden = (jax.nn.silu(gate_act) * up_act).astype(jnp.bfloat16)
        summed = jnp.zeros((rows_in.shape[0], D), jnp.float32)
        for block_number in range(N_TP):
            lower = block_number * block_width
            down_part = jnp.dot(hidden[:, lower:lower + block_width], down_matrix[lower:lower + block_width], preferred_element_type=jnp.float32)
            rounded = lax.optimization_barrier(down_part.astype(jnp.bfloat16))
            summed = summed + rounded.astype(jnp.float32)
        return summed.astype(jnp.bfloat16)
    expert_out = lax.map(one_expert, (buffer, w_gate, w_up, w_down)).reshape(slot_total, D)
    combined = jnp.zeros((TOKENS, D), jnp.float32)
    for column in range(TOP):
        picked = jnp.take(expert_out, flat_index[:, column], axis=0, mode='fill', fill_value=0).astype(jnp.float32)
        combined = combined + gate_prob[:, column:column + 1].astype(jnp.float32) * picked
    return combined.astype(jnp.bfloat16)
```

```python
import jax
import jax.numpy as jnp
from jax import lax
from jax.experimental import pallas as pl
from jax.experimental.pallas import tpu as pltpu
from jax.sharding import PartitionSpec as P

TOP = 8
EXP_DEV = 8
LANE = 128
FORTH = (4, 4, 6)
BACK = (6, 4, 4)


epsilon = 1e-06


def place_picks(expert_ids, gate_prob, window, capacity):
    is_live = expert_ids < window
    matches = (expert_ids[:, :, None] == jnp.arange(window, dtype=jnp.int32)).astype(jnp.int32)
    counts = jnp.sum(matches, axis=1)
    before = jnp.cumsum(counts, axis=0) - counts
    slot_index = jnp.sum(matches * before[:, None, :], axis=2)
    is_kept = is_live & (slot_index < capacity)
    target = jnp.where(is_kept, expert_ids * capacity + slot_index, -1)
    hit_table = target[:, :, None] == jnp.arange(window * capacity, dtype=jnp.int32)
    dispatch_mat = jnp.any(hit_table, axis=1).astype(jnp.bfloat16)
    weight_mat = jnp.sum(
        jnp.where(hit_table, gate_prob.astype(jnp.float32)[:, :, None], 0.0), axis=1
    ).astype(jnp.bfloat16)
    return (dispatch_mat, weight_mat)


def cuts(width, parts):
    units, total = width // LANE, sum(parts)
    edges, run = [0], 0
    for part in parts:
        run += part
        edges.append(units * run // total * LANE)
    edges[-1] = width
    return [(lo, hi) for lo, hi in zip(edges[:-1], edges[1:]) if hi > lo]


def ring(n_tp, shift):
    return [(i, (i + shift) % n_tp) for i in range(n_tp)]


def gate_up(chunks, starts, w_gate, w_up, sums, width, n_tp, last):
    count, units = chunks[0].shape[0], w_gate.shape[1]
    span = sum(rows.shape[1] for rows in chunks)
    pieces, base = [], 0
    for index, (rows, lo) in enumerate(zip(chunks, starts)):
        wide = rows.shape[1] // n_tp
        for z in range(n_tp):
            pieces.append((index, z * wide, wide, z, lo, base))
            base += wide

    def body(*refs):
        rows_refs, (gate_hbm, up_hbm) = refs[: len(chunks)], refs[len(chunks) : len(chunks) + 2]
        refs = refs[len(chunks) + 2 :]
        olds, outs = refs[: len(sums)], refs[len(sums) : -3]
        buffer, acc, sems = refs[-3:]
        copies = {}
        for p, (_, _, wide, z, lo, at) in enumerate(pieces):
            row = z * width + lo
            for m, source in enumerate((gate_hbm, up_hbm)):
                copies[m, p] = pltpu.make_async_copy(
                    source.at[pl.ds(row, wide)], buffer.at[m, pl.ds(at, wide)], sems.at[m, p]
                )
                copies[m, p].start()
        for p, (index, column, wide, _, _, at) in enumerate(pieces):
            for m in range(2):
                copies[m, p].wait()
                part = jnp.dot(
                    rows_refs[index][:, column : column + wide],
                    buffer[m, at : at + wide],
                    preferred_element_type=jnp.float32,
                )
                if p > 0:
                    part = acc[m] + part
                elif sums:
                    part = olds[m][...] + part
                acc[m] = part
        if last:
            gate_act = acc[0]
            outs[0][...] = (gate_act / (1.0 + jnp.exp(-gate_act)) * acc[1]).astype(jnp.bfloat16)
        else:
            outs[0][...] = acc[0]
            outs[1][...] = acc[1]

    if last:
        out_shape = [jax.ShapeDtypeStruct((count, units), jnp.bfloat16)]
    else:
        out_shape = [jax.ShapeDtypeStruct((count, units), jnp.float32)] * 2
    vmem = pl.BlockSpec(memory_space=pltpu.VMEM)
    hbm = pl.BlockSpec(memory_space=pl.ANY)
    return pl.pallas_call(
        body,
        out_shape=out_shape,
        in_specs=[vmem] * len(chunks) + [hbm, hbm] + [vmem] * len(sums),
        out_specs=[vmem] * len(out_shape),
        scratch_shapes=[
            pltpu.VMEM((2, span, units), w_gate.dtype),
            pltpu.VMEM((2, count, units), jnp.float32),
            pltpu.SemaphoreType.DMA((2, len(pieces))),
        ],
        cost_estimate=pl.CostEstimate(
            flops=4 * count * span * units,
            bytes_accessed=2 * (count * span + 2 * span * units + 4 * count * units),
            transcendentals=0,
        ),
    )(*chunks, w_gate, w_up, *sums)


def down_columns(hidden, w_down, lo, hi, width, n_tp):
    count, units = hidden.shape
    wide = hi - lo

    def body(hidden_ref, down_hbm, out_ref, buffer, sems):
        copies = []
        for z in range(n_tp):
            copies.append(
                pltpu.make_async_copy(
                    down_hbm.at[:, pl.ds(z * width + lo, wide)], buffer.at[z], sems.at[z]
                )
            )
            copies[z].start()
        for z in range(n_tp):
            copies[z].wait()
            part = jnp.dot(hidden_ref[...], buffer[z], preferred_element_type=jnp.float32)
            out_ref[:, z * wide : (z + 1) * wide] = part.astype(jnp.bfloat16)

    vmem = pl.BlockSpec(memory_space=pltpu.VMEM)
    return pl.pallas_call(
        body,
        out_shape=jax.ShapeDtypeStruct((count, n_tp * wide), jnp.bfloat16),
        in_specs=[vmem, pl.BlockSpec(memory_space=pl.ANY)],
        out_specs=vmem,
        scratch_shapes=[
            pltpu.VMEM((n_tp, units, wide), w_down.dtype),
            pltpu.SemaphoreType.DMA((n_tp,)),
        ],
        cost_estimate=pl.CostEstimate(
            flops=2 * count * units * n_tp * wide,
            bytes_accessed=2 * (count * units + (count + units) * n_tp * wide),
            transcendentals=0,
        ),
    )(hidden, w_down)


def local(tokens, norm_gain, expert_ids, gate_prob, w_gate, w_up, w_down):
    window = lax.axis_size("ep")
    n_tp = lax.axis_size("tp")
    tok_rows, width = tokens.shape
    capacity = max(2, 2 * tok_rows * TOP // (EXP_DEV * window))
    slots = window * capacity
    w_gate, w_up, w_down = w_gate[0], w_up[0], w_down[0]

    first, *rest = cuts(width, FORTH)

    values = tokens.astype(jnp.float32)
    gained = (values * norm_gain.astype(jnp.float32)[None, :]).astype(jnp.bfloat16)
    gathered = [
        lax.all_gather(gained[:, lo:hi], "tp", axis=1, tiled=True) for lo, hi in rest
    ]
    own = jnp.sum(values * values, axis=1).reshape(1, -1)
    total = own
    for shift in range(1, n_tp):
        total = total + lax.ppermute(own, "tp", ring(n_tp, shift))
    scale = lax.rsqrt(total.reshape(-1, 1) / (width * n_tp) + epsilon)

    dispatch_mat, weight_mat = place_picks(expert_ids, gate_prob, window, capacity)

    def dispatch(rows):
        scaled = (rows.astype(jnp.float32) * scale).astype(jnp.bfloat16)
        out = jnp.einsum("tp,td->pd", dispatch_mat, scaled, preferred_element_type=jnp.float32)
        out = out.astype(jnp.bfloat16).reshape(window, capacity, -1)
        back = lax.all_to_all(out, "ep", split_axis=0, concat_axis=0, tiled=True)
        return back.reshape(slots, -1)

    received = [dispatch(gained[:, first[0] : first[1]])]
    received[0] = lax.all_gather(received[0], "tp", axis=1, tiled=True)
    for rows in gathered:
        received.append(dispatch(rows))

    order = list(zip(rest, received[1:])) + [(first, received[0])]
    sums = ()
    for group in (order[:1], order[1:]):
        chunks = [rows for _, rows in group]
        starts = [lo for (lo, _), _ in group]
        sums = gate_up(chunks, starts, w_gate, w_up, sums, width, n_tp, len(sums) > 0)
    hidden = sums[0]

    def down(lo, hi):
        return down_columns(hidden, w_down, lo, hi, width, n_tp)

    back_first, *back_rest = cuts(width, BACK)

    def give_back(rows):
        shares = rows.reshape(window, capacity, -1)
        back = lax.all_to_all(shares, "ep", split_axis=0, concat_axis=0, tiled=True)
        back = back.reshape(slots, -1)
        out = jnp.einsum("tp,pd->td", weight_mat, back, preferred_element_type=jnp.float32)
        return out.astype(jnp.bfloat16)

    def scatter(rows):
        return lax.psum_scatter(rows, "tp", scatter_dimension=1, tiled=True)

    def scatter_direct(rows):
        wide, me = rows.shape[1] // n_tp, lax.axis_index("tp")
        total = 0.0
        for shift in range(n_tp):
            part = lax.dynamic_slice_in_dim(rows, (me + shift) % n_tp * wide, wide, axis=1)
            if shift > 0:
                part = lax.ppermute(part, "tp", ring(n_tp, shift))
            total = total + part.astype(jnp.float32)
        return total.astype(jnp.bfloat16)

    head = scatter(down(*back_first))
    tails = [scatter(give_back(down(lo, hi))) for lo, hi in back_rest[:-1]]
    tails.append(scatter_direct(give_back(down(*back_rest[-1]))))
    return jnp.concatenate([give_back(head)] + tails, axis=1)


def solution(mesh):
    placed = (
        P("ep", "tp"),
        P("tp"),
        P("ep", None),
        P("ep", None),
        P("ep", None, "tp"),
        P("ep", None, "tp"),
        P("ep", "tp", None),
    )
    return jax.shard_map(
        local, mesh=mesh, in_specs=placed, out_specs=P("ep", "tp"), check_vma=False
    )
```
